256 devices in a mesh: fft: 16 (over z, x_lo), pair: 16 (over y, x_hi, core).
Axes of the slice: x: 4 (x_hi: 2, x_lo: 2; x = x_hi * 2 + x_lo), y: 4, z: 8, core: 2. Of those that a mesh axis runs over, the one named last changes fastest.
Arguments:
- virt_orbitals: bfloat16 [1024, 96, 9216], P('pair', 'fft'), may hold values from -6 to 6
- occ_orbitals: bfloat16 [8, 96, 9216], P(None, 'fft'), may hold values from -6 to 6
- occ_index: int32 [1], replicated, may hold values from 0 to 7
- occ_energy: float32 [8], replicated, may hold values from -1.2 to -0.3
- band_energy: float32 [1024], replicated, may hold values from 0.1 to 3
- geminal_exponent: float32 [1], replicated, may hold values from 1.5 to 4
- pencil_index: int32 [1536], replicated, may hold values from 0 to 4703, as said below
- block_owner: int32 [16], replicated, may hold values from 0 to 15, each once
Outputs:
- pair_matrix: float32 [1024, 1024], P('pair', 'fft')
The draws below stay inside these ranges and needn't reach their ends.
Inputs may be any that keep to these rules, and one draw needn't show every extreme that they name: `pencil_index`: distinct and ascending; entry n names the pencil of second frequency pencil_index[n] // 49 and third frequency pencil_index[n] % 49 - 24. `block_owner`: a permutation of the band blocks.
All inputs are finite; a program needn't handle non-finite values.
Results may differ from the reference program's by a relative error of at most 0.0015.
The reference program's roundings to bfloat16 on the way (of `density`) count: a program that leaves them out, or rounds other values in their place, can miss the bound.
Values may be sent and summed in bfloat16 or wider, within the bound.
No kernel may reach another device: no remote copies, remote signals or barrier semaphores. Data moves between devices by JAX's collectives and lax.ppermute only.
A program may use at most 128 MiB of HBM per device.

```python
import math
import jax
import jax.numpy as jnp
from jax import lax

G = 96
R = 24
KZ = 49
NPEN = 1536
NBAND = 1024
OCC_ALL = 8
OCC = 1
BLOCKS = 16
N_PAIR = 16


def draw_pencil_index(key, part):
    key_one, key_two, key_three = jax.random.split(jax.random.fold_in(key, 17), 3)
    shift_y = jax.random.randint(key_one, (), -1, 2)
    shift_z = jax.random.randint(key_two, (), -1, 2)
    flat_index = jnp.arange(G * KZ, dtype=jnp.int32)
    freq_y = jnp.mod(flat_index // KZ + G // 2, G) - G // 2
    freq_z = flat_index % KZ - R
    distance = (2 * freq_y - shift_y) * (2 * freq_y - shift_y) + (2 * freq_z - shift_z) * (2 * freq_z - shift_z)
    tie_ranks = jax.random.permutation(key_three, G * KZ).astype(jnp.int32)
    scores = distance * (G * KZ) + tie_ranks
    ordering = jnp.argsort(scores, stable=True)
    return jnp.sort(ordering[:NPEN]).astype(jnp.int32)


def shard_levels(stream_key, extent, pieces, least, high):
    def one(axis_at, parts):
        draws = jax.random.uniform(jax.random.fold_in(jax.random.fold_in(stream_key, 6), axis_at), (parts,), jnp.float32, least / len(pieces), high / len(pieces))
        return jnp.repeat(jnp.exp(draws), extent[axis_at] // parts).reshape((-1,) + (1,) * (len(extent) - axis_at - 1))

    loudness = one(*pieces[0])
    for cut in pieces[1:]:
        loudness = loudness * one(*cut)
    return loudness


def scatter_about(key, dims, deviation, bound, shards=(), kind=jnp.bfloat16):
    drawn = deviation * jax.random.normal(key, dims, jnp.float32)
    if shards:
        drawn = drawn * shard_levels(key, dims, shards, -0.22, 0.18)
    return jnp.clip(drawn, -bound, bound).astype(kind)


def setup_inputs(seed: int = 0) -> dict:
    splits = jax.random.split(jax.random.key(seed), 9)
    return {
        "virt_orbitals": scatter_about(splits[0], (NBAND, G, G * G), 1.0, 6.0, ((0, 16), (1, 16))),
        "occ_orbitals": scatter_about(splits[1], (OCC_ALL, G, G * G), 1.0, 6.0, ((1, 16),)),
        "occ_index": jax.random.randint(splits[2], (OCC,), 0, OCC_ALL).astype(jnp.int32),
        "occ_energy": jnp.clip(jax.random.uniform(splits[3], (OCC_ALL,), jnp.float32, -1.2, -0.3), -1.2, -0.3),
        "band_energy": jnp.clip(jax.random.uniform(splits[4], (NBAND,), jnp.float32, 0.1, 3.0), 0.1, 3.0),
        "geminal_exponent": jnp.clip(jnp.exp(jax.random.uniform(splits[5], (1,), jnp.float32, math.log(1.5), math.log(4.0))), 1.5, 4.0),
        "pencil_index": draw_pencil_index(jax.random.fold_in(splits[8], 71), 0),
        "block_owner": jax.random.permutation(splits[7], BLOCKS).astype(jnp.int32),
    }


def phase_tables(length, offset, columns):
    grid_rows = jnp.arange(length, dtype=jnp.int32)[:, None]
    grid_cols = jnp.arange(columns, dtype=jnp.int32)[None, :] - offset
    turns = jnp.mod(grid_rows * grid_cols, length).astype(jnp.float32)
    angle = turns * (2.0 * math.pi / length)
    return jnp.cos(angle), jnp.sin(angle)


def forward_tables():
    cos_z, sin_z = phase_tables(G, R, KZ)
    z_table = jnp.concatenate([cos_z, -sin_z], axis=1).astype(jnp.bfloat16)
    cos_g, sin_g = phase_tables(G, 0, G)
    return z_table, cos_g.astype(jnp.bfloat16), sin_g.astype(jnp.bfloat16)


def half_kernel(exponent, kept_pens):
    freq_x = jnp.mod(jnp.arange(G, dtype=jnp.int32) + G // 2, G) - G // 2
    freq_y = jnp.mod(kept_pens // KZ + G // 2, G) - G // 2
    freq_z = kept_pens % KZ - R
    squared = (freq_x * freq_x)[:, None] + (freq_y * freq_y + freq_z * freq_z)[None, :]
    squared = squared.astype(jnp.float32)
    return 1.0 / ((G * exponent) ** 1.5 * (1.0 + squared / (exponent * exponent)))


def plane_coefficients(virtual, occupied, z_table, cos_g, sin_g, pencils):
    bands, planes = virtual.shape[0], virtual.shape[1]
    density = (occupied.astype(jnp.float32)[None] * virtual.astype(jnp.float32)).astype(jnp.bfloat16)
    z_coeffs = jnp.dot(density.reshape(bands * planes * G, G).astype(jnp.float32), z_table.astype(jnp.float32), preferred_element_type=jnp.float32)
    z_coeffs = z_coeffs.astype(jnp.bfloat16).astype(jnp.float32).reshape(bands * planes, G, 2 * KZ)
    cos_terms = jnp.einsum('myj,yk->mkj', z_coeffs, cos_g.astype(jnp.float32))
    sin_terms = jnp.einsum('myj,yk->mkj', z_coeffs, sin_g.astype(jnp.float32))
    real_part = (cos_terms[..., :KZ] + sin_terms[..., KZ:]).astype(jnp.bfloat16)
    imag_part = (cos_terms[..., KZ:] - sin_terms[..., :KZ]).astype(jnp.bfloat16)
    real_part = jnp.take(real_part.reshape(bands, planes, G * KZ), pencils, axis=2)
    imag_part = jnp.take(imag_part.reshape(bands, planes, G * KZ), pencils, axis=2)
    return real_part, imag_part


def spectral(real_part, imag_part, cos_g, sin_g, weight):
    columns = real_part.shape[-1]
    stacked = jnp.concatenate([real_part, imag_part], axis=-1).astype(jnp.float32)
    cos_terms = jnp.einsum('...xn,xk->...kn', stacked, cos_g.astype(jnp.float32))
    sin_terms = jnp.einsum('...xn,xk->...kn', stacked, sin_g.astype(jnp.float32))
    weighted_re = ((cos_terms[..., :columns] + sin_terms[..., columns:]) * weight).astype(jnp.bfloat16)
    weighted_im = ((cos_terms[..., columns:] - sin_terms[..., :columns]) * weight).astype(jnp.bfloat16)
    return weighted_re, weighted_im


def reference(virt_orbitals, occ_orbitals, occ_index, occ_energy, band_energy, geminal_exponent, pencil_index, block_owner):
    z_table, cos_g, sin_g = forward_tables()
    weight = half_kernel(geminal_exponent[0], pencil_index)
    spans = virt_orbitals.reshape(16, NBAND // 16, G, G * G)
    combined = jnp.zeros((NBAND, NBAND), jnp.float32)
    for number in range(OCC):
        occupied = occ_orbitals[occ_index[number]]

        def one_span(virtual):
            real_part, imag_part = plane_coefficients(virtual, occupied, z_table, cos_g, sin_g, pencil_index)
            return spectral(real_part, imag_part, cos_g, sin_g, weight)

        span_re, span_im = lax.map(one_span, spans)
        flat_re = span_re.reshape(NBAND, G * NPEN).astype(jnp.float32)
        flat_im = span_im.reshape(NBAND, G * NPEN).astype(jnp.float32)
        gram = jnp.dot(flat_re, flat_re.T, preferred_element_type=jnp.float32)
        gram = gram + jnp.dot(flat_im, flat_im.T, preferred_element_type=jnp.float32)
        factor = band_energy[:, None] + band_energy[None, :] - 2.0 * occ_energy[occ_index[number]]
        combined = combined + factor * gram
    arranged = jnp.take(combined.reshape(N_PAIR, NBAND // N_PAIR, NBAND), block_owner, axis=0)
    return arranged.reshape(NBAND, NBAND)
```

```python
import math

import jax
import jax.numpy as jnp
import numpy as np
from jax import lax
from jax.experimental import pallas as pl
from jax.experimental.pallas import tpu as pltpu
from jax.sharding import PartitionSpec as P

G = 96
R = 24
KZ = 49
NPEN = 1536
NBAND = 1024
FFT = 16
PAIR = 16
BANDS = NBAND // PAIR
PLANES = G // FFT
PENS = NPEN // (FFT * PAIR)
ROWS = 40
STEP = 16
NJ = R + 1


def rounded_tables():
    turns = (np.arange(G)[:, None] * np.arange(G)[None, :]) % G
    angle = turns.astype(np.float32) * np.float32(2.0 * math.pi / G)
    return np.cos(angle), np.sin(angle)


def z_stage_table():
    cos, sin = rounded_tables()
    table = np.zeros((NJ, 2, 8, 8, G), np.float32)
    for y in range(8):
        table[:, 0, y, y] = cos[:NJ]
        table[:, 1, y, y] = -sin[:NJ]
    return table.reshape(NJ * 2 * 8, 8 * G)


def y_stage_table():
    cos, sin = rounded_tables()
    return np.block([[cos, sin], [-sin, cos]])


def x_stage_table():
    cos, sin = rounded_tables()
    table = np.zeros((2, G, 2, FFT, ROWS), np.float32)
    for low in range(2):
        for source in range(FFT):
            for pencil in range(PENS):
                for high in range(3):
                    x = source * PLANES + 2 * high + low
                    for part in range(2):
                        row = pencil * 6 + part * 3 + high
                        if part == 0:
                            table[0, :, low, source, row] = cos[x]
                            table[1, :, low, source, row] = -sin[x]
                        else:
                            table[0, :, low, source, row] = sin[x]
                            table[1, :, low, source, row] = cos[x]
    return table.reshape(2 * G, 2 * FFT * ROWS)


def plane_kernel(occ_index, slots, virtual, occupied, z_table, y_table, out, z_parts, coeffs):
    step = pl.program_id(0)
    chosen = lax.broadcasted_iota(jnp.int32, (PLANES, 8, STEP * G), 1) == occ_index[0]
    orbital = jnp.sum(
        jnp.where(chosen, occupied[...].astype(jnp.float32), 0.0), axis=1, keepdims=True
    )
    pieces = []
    for half in range(2):
        lanes = slice(half * 8 * G, (half + 1) * 8 * G)
        density = (virtual[:, :, lanes].astype(jnp.float32) * orbital[:, :, lanes]).astype(
            jnp.bfloat16
        )
        density = density.reshape(PLANES * BANDS, 8 * G)
        z_coeffs = lax.dot_general(
            z_table[...], density, (((1,), (1,)), ((), ())), preferred_element_type=jnp.float32
        )
        pieces.append(z_coeffs.reshape(NJ * 2, 8, PLANES * BANDS))
    z_parts[:, pl.ds(pl.multiple_of(step * STEP, STEP), STEP), :] = jnp.concatenate(
        pieces, axis=1
    ).astype(jnp.bfloat16)

    @pl.when(step == pl.num_programs(0) - 1)
    def _():
        def one_frequency(j, carry):
            both = z_parts[pl.ds(2 * j, 2)].reshape(2 * G, PLANES * BANDS)
            values = jnp.dot(y_table[...], both, preferred_element_type=jnp.float32)
            for part in range(2):
                for high in range(3):
                    coeffs[pl.ds(j * (G * 8) + part * 3 + high, G, stride=8), :] = values[
                        part * G : (part + 1) * G, high * 128 : (high + 1) * 128
                    ]
            return carry

        lax.fori_loop(0, NJ, one_frequency, 0)

        def one_target(target, carry):
            rows = []
            for pencil in range(PENS):
                slot = slots[target * PENS + pencil]
                rows.append(coeffs[pl.ds(pl.multiple_of(slot * 8, 8), 8), :][:6])
            rows.append(jnp.zeros((ROWS - 6 * PENS, 128), jnp.float32))
            out[target] = jnp.concatenate(rows, axis=0).astype(jnp.bfloat16)
            return carry

        lax.fori_loop(0, FFT * PAIR, one_target, 0, unroll=4)


def plane_chunks(virtual, occupied, occ_index, slots):
    return pl.pallas_call(
        plane_kernel,
        grid_spec=pltpu.PrefetchScalarGridSpec(
            num_scalar_prefetch=2,
            grid=(G // STEP,),
            in_specs=[
                pl.BlockSpec((PLANES, BANDS, STEP * G), lambda s, *_: (0, 0, s)),
                pl.BlockSpec((PLANES, 8, STEP * G), lambda s, *_: (0, 0, s)),
                pl.BlockSpec((NJ * 16, 8 * G), lambda s, *_: (0, 0)),
                pl.BlockSpec((2 * G, 2 * G), lambda s, *_: (0, 0)),
            ],
            out_specs=pl.BlockSpec((FFT * PAIR, ROWS, 128), lambda s, *_: (0, 0, 0)),
            scratch_shapes=[
                pltpu.VMEM((NJ * 2, G, PLANES * BANDS), jnp.bfloat16),
                pltpu.VMEM((NJ * G * 8, 128), jnp.float32),
            ],
        ),
        out_shape=jax.ShapeDtypeStruct((FFT * PAIR, ROWS, 128), jnp.bfloat16),
        compiler_params=pltpu.CompilerParams(vmem_limit_bytes=56 * 1024 * 1024),
        name="planes",
    )(
        occ_index,
        slots,
        virtual,
        occupied,
        jnp.asarray(z_stage_table(), jnp.bfloat16),
        jnp.asarray(y_stage_table(), jnp.bfloat16),
    )


def swap_halves(first, second, low):
    left = jnp.where(low, first, pltpu.roll(second, 64, 1))
    right = jnp.where(low, pltpu.roll(first, 64, 1), second)
    return left, right


def gram_kernel(places, plane_freq, signs, scale, arrived, x_table, mine, theirs, stacked, spectra):
    for pair in range(PAIR // 2):
        first = arrived[:, 2 * pair].astype(jnp.float32).reshape(FFT * ROWS, 128)
        second = arrived[:, 2 * pair + 1].astype(jnp.float32).reshape(FFT * ROWS, 128)
        low = lax.broadcasted_iota(jnp.int32, (FFT * ROWS, 128), 1) < 64
        left, right = swap_halves(first, second, low)
        lanes = slice(pair * 128, (pair + 1) * 128)
        stacked[0 : FFT * ROWS, lanes] = left.astype(jnp.bfloat16)
        stacked[FFT * ROWS :, lanes] = right.astype(jnp.bfloat16)

    freq = lax.broadcasted_iota(jnp.int32, (2 * G, 128), 0) % G
    freq = (freq + G // 2) % G - G // 2
    squared_x = freq * freq
    exponent = jnp.full((2 * G, 128), scale[0], jnp.float32)
    norm = exponent * G
    norm = norm * jnp.sqrt(norm)
    column = lax.broadcasted_iota(jnp.int32, (2 * G, 2 * FFT * ROWS), 1) % ROWS
    for pencil in range(PENS):
        squared = (squared_x + plane_freq[pencil]).astype(jnp.float32)
        weight = 1.0 / (norm * (1.0 + squared / (exponent * exponent)))
        sign = signs[pencil]
        factor = jnp.where(
            column // 3 == 2 * pencil,
            1.0,
            jnp.where(column // 3 == 2 * pencil + 1, sign, 0.0),
        ).astype(jnp.bfloat16)
        values = jnp.dot(x_table[...] * factor, stacked[...], preferred_element_type=jnp.float32)
        weight = jnp.concatenate([weight] * (NBAND // 128), axis=1)
        spectra[pencil * 2 * G : (pencil + 1) * 2 * G, :] = (values * weight).astype(jnp.bfloat16)

    low = lax.broadcasted_iota(jnp.int32, (BANDS // 2, 128), 1) < 64
    for group in range(4):
        gram = lax.dot_general(
            spectra[:, group * 256 : (group + 1) * 256],
            spectra[...],
            (((0,), (0,)), ((), ())),
            preferred_element_type=jnp.float32,
        )
        for inner in range(4):
            place = places[group * 4 + inner]
            parts = []
            for pair in range(PAIR // 2):
                tile = gram[inner * 64 : (inner + 1) * 64, pair * 128 : (pair + 1) * 128]
                parts.extend(swap_halves(tile[:32], tile[32:], low))

            @pl.when(place < PAIR // 2)
            def _():
                for part in range(PAIR):
                    mine[place, part] = parts[part]

            @pl.when(place >= PAIR // 2)
            def _():
                for part in range(PAIR):
                    theirs[place - PAIR // 2, part] = parts[part]


def gram_halves(places, plane_freq, signs, scale, arrived):
    half = jax.ShapeDtypeStruct((PAIR // 2, PAIR, 32, 128), jnp.float32)
    smem = pl.BlockSpec(memory_space=pltpu.SMEM)
    vmem = pl.BlockSpec(memory_space=pltpu.VMEM)
    return pl.pallas_call(
        gram_kernel,
        in_specs=[smem, smem, smem, smem, vmem, vmem],
        out_specs=[vmem, vmem],
        out_shape=[half, half],
        scratch_shapes=[
            pltpu.VMEM((2 * FFT * ROWS, NBAND), jnp.bfloat16),
            pltpu.VMEM((PENS * 2 * G, NBAND), jnp.bfloat16),
        ],
        compiler_params=pltpu.CompilerParams(vmem_limit_bytes=56 * 1024 * 1024),
        name="gram",
    )(
        places,
        plane_freq,
        signs,
        scale,
        arrived.reshape(FFT, PAIR, ROWS, 128),
        jnp.asarray(x_stage_table(), jnp.bfloat16),
    )


def body(
    virt_orbitals,
    occ_orbitals,
    occ_index,
    occ_energy,
    band_energy,
    geminal_exponent,
    pencil_index,
    block_owner,
):
    fft_at = lax.axis_index("fft")
    pair_at = lax.axis_index("pair")
    k = pencil_index // KZ
    j = pencil_index % KZ - R
    slots = jnp.abs(j) * G + jnp.where(j >= 0, k, (G - k) % G)
    chunks = plane_chunks(
        jnp.transpose(virt_orbitals, (1, 0, 2)),
        jnp.transpose(occ_orbitals, (1, 0, 2)),
        occ_index,
        slots,
    )
    arrived = lax.all_to_all(chunks, ("fft", "pair"), split_axis=0, concat_axis=0, tiled=True)

    start = (fft_at * PAIR + pair_at) * PENS
    kept = lax.dynamic_slice_in_dim(pencil_index, start, PENS)
    freq_y = (kept // KZ + G // 2) % G - G // 2
    freq_z = kept % KZ - R
    signs = jnp.where(freq_z >= 0, 1.0, -1.0).astype(jnp.float32)
    order = jnp.arange(PAIR, dtype=jnp.int32)
    owner = jnp.sum(
        jnp.where(block_owner[:, None] == order[None, :], order[:, None], 0), axis=0
    )
    places = owner // 2 + jnp.where(owner % 2 == pair_at % 2, 0, PAIR // 2)
    mine, theirs = gram_halves(
        places, freq_y * freq_y + freq_z * freq_z, signs, geminal_exponent, arrived
    )
    swapped = lax.ppermute(theirs, "pair", [(i, i ^ 1) for i in range(PAIR)])
    same_core = [list(range(0, PAIR, 2)), list(range(1, PAIR, 2))]
    rows = lax.all_to_all(
        mine + swapped, "pair", 0, 0, tiled=True, axis_index_groups=same_core
    ).sum(axis=0)
    total = lax.all_to_all(rows, "fft", 0, 0, tiled=True).sum(axis=0)
    gram = jnp.concatenate([total[:, :64], total[:, 64:]], axis=0)
    block = lax.dynamic_index_in_dim(block_owner, pair_at, keepdims=False)
    row_energy = lax.dynamic_slice_in_dim(band_energy, block * BANDS, BANDS)
    column_energy = lax.dynamic_slice_in_dim(band_energy, fft_at * BANDS, BANDS)
    occupied_energy = lax.dynamic_index_in_dim(occ_energy, occ_index[0], keepdims=False)
    return (row_energy[:, None] + column_energy[None, :] - 2.0 * occupied_energy) * gram


def solution(mesh):
    return jax.shard_map(
        body,
        mesh=mesh,
        in_specs=(P("pair", "fft", None), P(None, "fft", None), P(), P(), P(), P(), P(), P()),
        out_specs=P("pair", "fft"),
        check_vma=False,
    )
```

```python
import math

import jax
import jax.numpy as jnp
import numpy as np
from jax import lax
from jax.experimental import pallas as pl
from jax.experimental.pallas import tpu as pltpu
from jax.sharding import PartitionSpec as P

G = 96
R = 24
KZ = 49
NPEN = 1536
NBAND = 1024
FFT = 16
PAIR = 16
BANDS = NBAND // PAIR
PLANES = G // FFT
FIRST = 4
SECOND = NPEN // (FFT * PAIR) - FIRST
DEVICES = FFT * PAIR
FIRST_ROWS = 6 * FIRST
SECOND_ROWS = 16
STEP = 16
NJ = R + 1
POINTS = PLANES * BANDS


def rounded_tables():
    turns = (np.arange(G)[:, None] * np.arange(G)[None, :]) % G
    angle = turns.astype(np.float32) * np.float32(2.0 * math.pi / G)
    return np.cos(angle), np.sin(angle)


def z_stage_tables():
    cos, sin = rounded_tables()
    table = np.zeros((2, NJ, 2, 4, 4, G), np.float32)
    for y in range(4):
        for odd in range(2):
            table[odd, :, odd, y, y] = cos[:NJ]
            table[odd, :, 1 - odd, y, y] = -sin[:NJ]
    return table.reshape(2, NJ * 8, 4 * G)


def y_stage_table():
    cos, sin = rounded_tables()
    swapped = np.arange(G).reshape(-1, 2, 4)[:, ::-1].reshape(-1)
    return np.block([[cos, sin[:, swapped]], [-sin, cos[:, swapped]]])


def x_stage_table(pencils, rows):
    cos, sin = rounded_tables()
    table = np.zeros((2, G, 2, FFT, rows), np.float32)
    for low in range(2):
        for source in range(FFT):
            for pencil in range(pencils):
                for high in range(3):
                    x = source * PLANES + 2 * high + low
                    row = pencil * 6 + high
                    table[0, :, low, source, row] = cos[x]
                    table[1, :, low, source, row] = -sin[x]
                    table[0, :, low, source, row + 3] = sin[x]
                    table[1, :, low, source, row + 3] = cos[x]
    return table.reshape(2 * G, 2 * FFT * rows)


def plan_kernel(pencils, slots, weights, squares, total):
    index = pencils[...]
    k = index // KZ
    j = index % KZ - R
    mirror = (G - k) % G
    folded = jnp.where(j > 0, k, jnp.where(j < 0, mirror, jnp.minimum(k, mirror)))
    k_rows = lax.broadcasted_iota(jnp.int32, (G, NPEN), 0)
    j_rows = lax.broadcasted_iota(jnp.int32, (32, NPEN), 0)
    k_hot = jnp.where(k_rows == folded, 1.0, 0.0).astype(jnp.bfloat16)
    j_hot = jnp.where(j_rows == jnp.abs(j), 1.0, 0.0).astype(jnp.bfloat16)
    contract_lanes = (((1,), (1,)), ((), ()))
    contract_rows = (((0,), (0,)), ((), ()))
    count = lax.dot_general(j_hot, k_hot, contract_lanes, preferred_element_type=jnp.float32)
    present = jnp.where(count > 0.5, 1.0, 0.0).astype(jnp.bfloat16)
    upto = jnp.where(
        lax.broadcasted_iota(jnp.int32, (G, G), 0) <= lax.broadcasted_iota(jnp.int32, (G, G), 1),
        1.0,
        0.0,
    ).astype(jnp.bfloat16)
    within = jnp.dot(present, upto, preferred_element_type=jnp.float32)
    before = jnp.where(
        lax.broadcasted_iota(jnp.int32, (32, 32), 1) < lax.broadcasted_iota(jnp.int32, (32, 32), 0),
        1.0,
        0.0,
    ).astype(jnp.bfloat16)
    column_total = within[:, G - 1 : G]
    column_wide = jnp.broadcast_to(column_total, (32, 128))
    start = jnp.dot(before, column_wide.astype(jnp.bfloat16), preferred_element_type=jnp.float32)
    start = start[:, 0:1]
    stop = start + column_total
    entry = lax.broadcasted_iota(jnp.int32, (1, NPEN), 1).astype(jnp.float32)
    past = entry >= stop
    column = jnp.sum(jnp.where(past, 1, 0), axis=0, keepdims=True)
    offset = jnp.sum(jnp.where(past, column_total, 0.0), axis=0, keepdims=True)
    own_column = jnp.where(j_rows == column, 1.0, 0.0).astype(jnp.bfloat16)
    own_within = lax.dot_general(
        within.astype(jnp.bfloat16), own_column, contract_rows, preferred_element_type=jnp.float32
    )
    own_count = lax.dot_general(
        count.astype(jnp.bfloat16), own_column, contract_rows, preferred_element_type=jnp.float32
    )
    row = jnp.sum(jnp.where(own_within <= entry - offset, 1, 0), axis=0, keepdims=True)
    weight = jnp.sum(jnp.where(k_rows == row, own_count, 0.0), axis=0, keepdims=True)
    valid = column < NJ
    row = jnp.minimum(row, G - 1)
    column = jnp.minimum(column, NJ - 1)
    signed = (row + G // 2) % G - G // 2
    slots[...] = jnp.where(valid, column * G + row, 0)
    weights[...] = jnp.where(valid, weight, 0.0)
    squares[...] = jnp.where(valid, signed * signed + column * column, 0)
    total[...] = jnp.broadcast_to(jnp.sum(column_total, axis=0, keepdims=True), (1, 128)).astype(jnp.int32)


def pencil_plan(pencil_index):
    vmem = pl.BlockSpec(memory_space=pltpu.VMEM)
    return pl.pallas_call(
        plan_kernel,
        in_specs=[vmem],
        out_specs=[vmem] * 4,
        out_shape=[
            jax.ShapeDtypeStruct((1, NPEN), jnp.int32),
            jax.ShapeDtypeStruct((1, NPEN), jnp.float32),
            jax.ShapeDtypeStruct((1, NPEN), jnp.int32),
            jax.ShapeDtypeStruct((1, 128), jnp.int32),
        ],
        name="plan",
    )(pencil_index.reshape(1, NPEN))


def plane_kernel(
    occ_index, slots, total, virtual, occupied, z_tables, y_table, out, more, z_parts, coeffs
):
    step = pl.program_id(0)
    chosen = lax.broadcasted_iota(jnp.int32, (PLANES, 8, STEP * G), 1) == occ_index[0]
    orbital = jnp.sum(
        jnp.where(chosen, occupied[...].astype(jnp.float32), 0.0), axis=1, keepdims=True
    )

    def density(group):
        lanes = slice(group * 4 * G, (group + 1) * 4 * G)
        product = virtual[:, :, lanes].astype(jnp.float32) * orbital[:, :, lanes]
        return product.astype(jnp.bfloat16).reshape(POINTS, 4 * G)

    halves = []
    for odd in range(2):
        halves.append(
            lax.dot_general(
                z_tables[odd],
                jnp.concatenate([density(odd), density(odd + 2)], axis=0),
                (((1,), (1,)), ((), ())),
                preferred_element_type=jnp.float32,
            ).reshape(NJ, 8, 2 * POINTS)
        )
    top = lax.broadcasted_iota(jnp.int32, (NJ, 8, POINTS), 1) < 4
    tiles = [[], []]
    for group in range(2):
        lanes = slice(group * POINTS, (group + 1) * POINTS)
        even, odd = halves[0][:, :, lanes], halves[1][:, :, lanes]
        tiles[0].append(jnp.where(top, even, odd))
        tiles[1].append(jnp.where(top, odd, even))
    here = pl.ds(pl.multiple_of(step * STEP, STEP), STEP)
    for part in range(2):
        z_parts[:, part, here, :] = jnp.concatenate(tiles[part], axis=1).astype(jnp.bfloat16)

    @pl.when(step == pl.num_programs(0) - 1)
    def _():
        def transform(j, width):
            both = [
                z_parts[j + one].reshape(2 * G, POINTS) for one in range(width)
            ]
            both = both[0] if width == 1 else jnp.concatenate(both, axis=1)
            values = jnp.dot(y_table[...], both, preferred_element_type=jnp.float32)
            for one in range(width):
                for part in range(2):
                    for high in range(3):
                        lane = one * POINTS + high * 128
                        place = (j + one) * (G * 8) + part * 3 + high
                        coeffs[pl.ds(place, G, stride=8), :] = values[
                            part * G : (part + 1) * G, lane : lane + 128
                        ]

        def two_frequencies(at, carry):
            transform(2 * at, 2)
            return carry

        lax.fori_loop(0, NJ // 2, two_frequencies, 0)
        transform(NJ - 1, 1)

        def fill(target_ref, first, pencils, rows, base):
            def one_target(target, carry):
                pieces = []
                for pencil in range(pencils):
                    slot = slots[0, base + target * pencils + pencil]
                    pieces.append(coeffs[pl.ds(pl.multiple_of(slot * 8, 8), 8), :][:6])
                if rows > 6 * pencils:
                    pieces.append(jnp.zeros((rows - 6 * pencils, 128), jnp.float32))
                target_ref[target] = jnp.concatenate(pieces, axis=0).astype(jnp.bfloat16)
                return carry

            lax.fori_loop(0, DEVICES, one_target, 0, unroll=first)

        fill(out, 8, FIRST, FIRST_ROWS, 0)

        @pl.when(total[0, 0] > DEVICES * FIRST)
        def _():
            fill(more, 1, SECOND, SECOND_ROWS, DEVICES * FIRST)


def plane_chunks(virtual, occupied, occ_index, slots, total):
    smem = pl.BlockSpec(memory_space=pltpu.SMEM)
    whole = lambda *shape: pl.BlockSpec(shape, lambda s: (0,) * len(shape))
    return pl.pallas_call(
        plane_kernel,
        grid=(G // STEP,),
        in_specs=[
            smem,
            smem,
            smem,
            pl.BlockSpec((PLANES, BANDS, STEP * G), lambda s: (0, 0, s)),
            pl.BlockSpec((PLANES, 8, STEP * G), lambda s: (0, 0, s)),
            whole(2, NJ * 8, 4 * G),
            whole(2 * G, 2 * G),
        ],
        out_specs=[whole(DEVICES, FIRST_ROWS, 128), whole(DEVICES, SECOND_ROWS, 128)],
        scratch_shapes=[
            pltpu.VMEM((NJ, 2, G, POINTS), jnp.bfloat16),
            pltpu.VMEM((NJ * G * 8, 128), jnp.float32),
        ],
        out_shape=[
            jax.ShapeDtypeStruct((DEVICES, FIRST_ROWS, 128), jnp.bfloat16),
            jax.ShapeDtypeStruct((DEVICES, SECOND_ROWS, 128), jnp.bfloat16),
        ],
        compiler_params=pltpu.CompilerParams(vmem_limit_bytes=56 * 1024 * 1024),
        name="planes",
    )(
        occ_index,
        slots,
        total,
        virtual,
        occupied,
        jnp.asarray(z_stage_tables(), jnp.bfloat16),
        jnp.asarray(y_stage_table(), jnp.bfloat16),
    )


def swap_halves(first, second, low):
    left = jnp.where(low, first, pltpu.roll(second, 64, 1))
    right = jnp.where(low, pltpu.roll(first, 64, 1), second)
    return left, right


def stack_sources(source, stacked, rows):
    count = FFT * rows
    low = lax.broadcasted_iota(jnp.int32, (count, 128), 1) < 64
    for pair in range(PAIR // 2):
        first = source[:, 2 * pair].astype(jnp.float32).reshape(count, 128)
        second = source[:, 2 * pair + 1].astype(jnp.float32).reshape(count, 128)
        left, right = swap_halves(first, second, low)
        lanes = slice(pair * 128, (pair + 1) * 128)
        stacked[0:count, lanes] = left.astype(jnp.bfloat16)
        stacked[count : 2 * count, lanes] = right.astype(jnp.bfloat16)


def gram_kernel(
    places,
    own,
    total,
    squares,
    weights,
    scale,
    arrived,
    later,
    x_table,
    later_table,
    mine,
    theirs,
    stacked,
    spectra,
    weighted,
    later_here,
    later_stacked,
    sem,
):
    freq = lax.broadcasted_iota(jnp.int32, (2 * G, 128), 0) % G
    freq = (freq + G // 2) % G - G // 2
    squared_x = freq * freq
    exponent = jnp.full((2 * G, 128), scale[0], jnp.float32)
    norm = exponent * G
    norm = norm * jnp.sqrt(norm)

    def transform(table, source, rows, pencils, base, at):
        column = lax.broadcasted_iota(jnp.int32, (2 * G, 2 * FFT * rows), 1) % rows
        for pencil in range(pencils):
            entry = base + pencil
            squared = (squared_x + squares[0, entry]).astype(jnp.float32)
            half = 1.0 / (norm * (1.0 + squared / (exponent * exponent)))
            chosen = jnp.where(column // 6 == pencil, 1.0, 0.0).astype(jnp.bfloat16)
            values = jnp.dot(table[...] * chosen, source[...], preferred_element_type=jnp.float32)
            half = jnp.concatenate([half] * (NBAND // 128), axis=1)
            here = slice((at + pencil) * 2 * G, (at + pencil + 1) * 2 * G)
            rounded = (values * half).astype(jnp.bfloat16)
            spectra[here, :] = rounded
            weighted[here, :] = rounded * jnp.full(
                rounded.shape, weights[0, entry], jnp.float32
            ).astype(jnp.bfloat16)

    stack_sources(arrived, stacked, FIRST_ROWS)
    transform(x_table, stacked, FIRST_ROWS, FIRST, own[0] * FIRST, 0)

    def multiply(pencils):
        low = lax.broadcasted_iota(jnp.int32, (BANDS // 2, 128), 1) < 64
        terms = pencils * 2 * G
        for group in range(4):
            gram = lax.dot_general(
                weighted[:terms, group * 256 : (group + 1) * 256],
                spectra[:terms, :],
                (((0,), (0,)), ((), ())),
                preferred_element_type=jnp.float32,
            )
            for inner in range(4):
                place = places[group * 4 + inner]
                parts = []
                for pair in range(PAIR // 2):
                    tile = gram[inner * 64 : (inner + 1) * 64, pair * 128 : (pair + 1) * 128]
                    parts.extend(swap_halves(tile[:32], tile[32:], low))

                @pl.when(place < PAIR // 2)
                def _():
                    for part in range(PAIR):
                        mine[place, part] = parts[part]

                @pl.when(place >= PAIR // 2)
                def _():
                    for part in range(PAIR):
                        theirs[place - PAIR // 2, part] = parts[part]

    @pl.when(total[0, 0] <= DEVICES * FIRST)
    def _():
        multiply(FIRST)

    @pl.when(total[0, 0] > DEVICES * FIRST)
    def _():
        copy = pltpu.make_async_copy(later, later_here, sem)
        copy.start()
        copy.wait()
        stack_sources(later_here, later_stacked, SECOND_ROWS)
        base = DEVICES * FIRST + own[0] * SECOND
        transform(later_table, later_stacked, SECOND_ROWS, SECOND, base, FIRST)
        multiply(FIRST + SECOND)


def gram_halves(places, own, total, squares, weights, scale, arrived, later):
    half = jax.ShapeDtypeStruct((PAIR // 2, PAIR, 32, 128), jnp.float32)
    smem = pl.BlockSpec(memory_space=pltpu.SMEM)
    vmem = pl.BlockSpec(memory_space=pltpu.VMEM)
    anywhere = pl.BlockSpec(memory_space=pl.ANY)
    terms = (FIRST + SECOND) * 2 * G
    return pl.pallas_call(
        gram_kernel,
        in_specs=[smem] * 6 + [vmem, anywhere, vmem, vmem],
        out_specs=[vmem, vmem],
        out_shape=[half, half],
        scratch_shapes=[
            pltpu.VMEM((2 * FFT * FIRST_ROWS, NBAND), jnp.bfloat16),
            pltpu.VMEM((terms, NBAND), jnp.bfloat16),
            pltpu.VMEM((terms, NBAND), jnp.bfloat16),
            pltpu.VMEM((FFT, PAIR, SECOND_ROWS, 128), jnp.bfloat16),
            pltpu.VMEM((2 * FFT * SECOND_ROWS, NBAND), jnp.bfloat16),
            pltpu.SemaphoreType.DMA,
        ],
        compiler_params=pltpu.CompilerParams(vmem_limit_bytes=56 * 1024 * 1024),
        name="gram",
    )(
        places,
        own,
        total,
        squares,
        weights,
        scale,
        arrived.reshape(FFT, PAIR, FIRST_ROWS, 128),
        later.reshape(FFT, PAIR, SECOND_ROWS, 128),
        jnp.asarray(x_stage_table(FIRST, FIRST_ROWS), jnp.bfloat16),
        jnp.asarray(x_stage_table(SECOND, SECOND_ROWS), jnp.bfloat16),
    )


def body(
    virt_orbitals,
    occ_orbitals,
    occ_index,
    occ_energy,
    band_energy,
    geminal_exponent,
    pencil_index,
    block_owner,
):
    fft_at = lax.axis_index("fft")
    pair_at = lax.axis_index("pair")
    slots, weights, squares, total = pencil_plan(pencil_index)
    chunks, more = plane_chunks(
        jnp.transpose(virt_orbitals, (1, 0, 2)),
        jnp.transpose(occ_orbitals, (1, 0, 2)),
        occ_index,
        slots,
        total,
    )

    def exchanged(sent):
        return lax.all_to_all(sent, ("fft", "pair"), split_axis=0, concat_axis=0, tiled=True)

    arrived = exchanged(chunks)
    later = lax.cond(total[0, 0] > DEVICES * FIRST, exchanged, jnp.zeros_like, more)

    order = jnp.arange(PAIR, dtype=jnp.int32)
    owner = jnp.sum(
        jnp.where(block_owner[:, None] == order[None, :], order[:, None], 0), axis=0
    )
    places = owner // 2 + jnp.where(owner % 2 == pair_at % 2, 0, PAIR // 2)
    own = jnp.reshape(fft_at * PAIR + pair_at, (1,))
    mine, theirs = gram_halves(
        places, own, total, squares, weights, geminal_exponent, arrived, later
    )
    swapped = lax.ppermute(theirs, "pair", [(i, i ^ 1) for i in range(PAIR)])
    same_core = [list(range(0, PAIR, 2)), list(range(1, PAIR, 2))]
    rows = lax.all_to_all(
        mine + swapped, "pair", 0, 0, tiled=True, axis_index_groups=same_core
    ).sum(axis=0)
    total = lax.all_to_all(rows, "fft", 0, 0, tiled=True).sum(axis=0)
    gram = jnp.concatenate([total[:, :64], total[:, 64:]], axis=0)
    block = lax.dynamic_index_in_dim(block_owner, pair_at, keepdims=False)
    row_energy = lax.dynamic_slice_in_dim(band_energy, block * BANDS, BANDS)
    column_energy = lax.dynamic_slice_in_dim(band_energy, fft_at * BANDS, BANDS)
    occupied_energy = lax.dynamic_index_in_dim(occ_energy, occ_index[0], keepdims=False)
    return (row_energy[:, None] + column_energy[None, :] - 2.0 * occupied_energy) * gram


def solution(mesh):
    return jax.shard_map(
        body,
        mesh=mesh,
        in_specs=(P("pair", "fft", None), P(None, "fft", None), P(), P(), P(), P(), P(), P()),
        out_specs=P("pair", "fft"),
        check_vma=False,
    )
```
